32 devices in a mesh: dp: 1 (over z), tp: 4 (over y), sp: 8 (over x, core).
Axes of the slice: x: 4, y: 4, z: 1, core: 2. Of those that a mesh axis runs over, the one named last changes fastest.
The devices are a block of a 4x4x8 slice.
Arguments:
- x_seq: bfloat16 [6144, 4096], P(('dp', 'sp', 'tp'))
- w_query: bfloat16 [4096, 32, 128], P(None, 'tp')
- w_key: bfloat16 [4096, 8, 128], P(None, 'tp')
- w_value: bfloat16 [4096, 8, 128], P(None, 'tp')
- w_out: bfloat16 [32, 128, 4096], P('tp')
Outputs:
- output: bfloat16 [6144, 4096], P(('dp', 'sp', 'tp'))
All inputs are finite; a program needn't handle non-finite values.
Results may differ from the reference program's by a relative error of at most 0.00855549.
Values are sent between devices in bfloat16 or wider.
A program may use at most 768 MiB of HBM per device.

```python
import jax
import jax.numpy as jnp
from jax import lax

D = 4096
HEADS = 32
KV_HEADS = 8
HEAD = 128
WINDOW = 4096
CHUNK = 384
SP = 8
QBLOCK = 128

SEQ = 2 * SP * CHUNK
GROUP = HEADS // KV_HEADS
SPAN = WINDOW + QBLOCK
NEG_BIG = -1e30


def setup_inputs(seed: int = 0, part: int = 0) -> dict:
    base_key = jax.random.key(seed)
    part_key = jax.random.fold_in(base_key, part)
    weight_keys = jax.random.split(base_key, 4)
    x_rows = jax.random.normal(part_key, (SEQ, D), jnp.float32)
    w_query = jax.random.normal(weight_keys[0], (D, HEADS, HEAD), jnp.float32) * (1.5 * D ** -0.5)
    w_key = jax.random.normal(weight_keys[1], (D, KV_HEADS, HEAD), jnp.float32) * D ** -0.5
    w_value = jax.random.normal(weight_keys[2], (D, KV_HEADS, HEAD), jnp.float32) * D ** -0.5
    w_out = jax.random.normal(weight_keys[3], (HEADS, HEAD, D), jnp.float32) * (HEADS * HEAD) ** -0.5
    return {"x_seq": x_rows.astype(jnp.bfloat16), "w_query": w_query.astype(jnp.bfloat16), "w_key": w_key.astype(jnp.bfloat16), "w_value": w_value.astype(jnp.bfloat16), "w_out": w_out.astype(jnp.bfloat16)}


def to_natural(rows_in):
    blocks = rows_in.reshape((SP, 2, CHUNK) + rows_in.shape[1:])
    return jnp.concatenate([blocks[:, 0], blocks[::-1, 1]], axis=0).reshape(rows_in.shape)


def to_stored(rows_in):
    blocks = rows_in.reshape((2 * SP, CHUNK) + rows_in.shape[1:])
    return jnp.stack([blocks[:SP], blocks[SP:][::-1]], axis=1).reshape(rows_in.shape)


def reference(x_seq, w_query, w_key, w_value, w_out):
    x_nat = to_natural(x_seq)
    q_all = jnp.dot(x_nat, w_query.reshape(D, HEADS * HEAD), preferred_element_type=jnp.float32).astype(jnp.bfloat16).reshape(SEQ, KV_HEADS, GROUP, HEAD)
    k_all = jnp.dot(x_nat, w_key.reshape(D, KV_HEADS * HEAD), preferred_element_type=jnp.float32).astype(jnp.bfloat16).reshape(SEQ, KV_HEADS, HEAD)
    v_all = jnp.dot(x_nat, w_value.reshape(D, KV_HEADS * HEAD), preferred_element_type=jnp.float32).astype(jnp.bfloat16).reshape(SEQ, KV_HEADS, HEAD)
    zero_front = jnp.zeros((WINDOW, KV_HEADS, HEAD), jnp.bfloat16)
    k_pad = jnp.concatenate([zero_front, k_all], axis=0)
    v_pad = jnp.concatenate([zero_front, v_all], axis=0)
    score_scale = HEAD ** -0.5
    row_ids = jnp.arange(QBLOCK)[:, None]
    col_ids = jnp.arange(SPAN)[None, :]

    def one_block(start):
        q_blk = lax.dynamic_slice_in_dim(q_all, start, QBLOCK, 0).astype(jnp.float32)
        k_blk = lax.dynamic_slice_in_dim(k_pad, start, SPAN, 0).astype(jnp.float32)
        v_blk = lax.dynamic_slice_in_dim(v_pad, start, SPAN, 0).astype(jnp.float32)
        scores = jnp.einsum("qhgd,khd->hgqk", q_blk, k_blk) * score_scale
        pos_gap = WINDOW + row_ids - col_ids
        visible = (pos_gap >= 0) & (pos_gap < WINDOW) & (start - WINDOW + col_ids >= 0)
        scores = jnp.where(visible, scores, NEG_BIG)
        row_max = jnp.max(scores, axis=-1, keepdims=True)
        prob_blk = jnp.where(visible, jnp.exp(scores - row_max), 0.0)
        row_denom = jnp.sum(prob_blk, axis=-1)
        weighted = jnp.einsum("hgqk,khd->hgqd", prob_blk.astype(jnp.bfloat16).astype(jnp.float32), v_blk)
        normed = (weighted / row_denom[..., None]).astype(jnp.bfloat16)
        return jnp.transpose(normed, (2, 0, 1, 3)).reshape(QBLOCK, HEADS * HEAD)

    starts = jnp.arange(SEQ // QBLOCK) * QBLOCK
    o_nat = lax.map(one_block, starts).reshape(SEQ, HEADS * HEAD)
    y_nat = jnp.dot(o_nat, w_out.reshape(HEADS * HEAD, D), preferred_element_type=jnp.float32).astype(jnp.bfloat16)
    return to_stored(y_nat)
```

```python
import functools

import jax
import jax.numpy as jnp
from jax import lax
from jax.experimental import pallas as pl
from jax.experimental.pallas import tpu as pltpu
from jax.sharding import PartitionSpec as P

WINDOW = 4096
NEG_BIG = -1e30
LOG2E = 1.4426950408889634
TILE = 256
MESH = pl.DeviceIdType.MESH
NT = (((1,), (1,)), ((), ()))
NN = (((1,), (0,)), ((), ()))


def attn_kernel(dims, q_ref, kv_in, o_ref, kv, m_s, l_s, acc_s, own_sem, send_sem, recv_sem):
    sp_size, chunk, head_dim, kv_loc, group = dims
    chips = sp_size // 2
    cols = group * chunk
    tiles = cols // TILE
    scale = head_dim ** -0.5 * LOG2E
    me = lax.axis_index("sp")
    core = lax.rem(me, 2)
    chip = me // 2

    def rank(dx, flip):
        c = core if flip == 0 else 1 - core
        return 2 * lax.rem(chip + dx + chips, chips) + c

    partner, right, left = rank(0, 1), rank(1, 0), rank(-1, 0)
    own = pltpu.make_async_copy(kv_in, kv.at[me], own_sem)
    own.start()
    barrier = pltpu.get_barrier_semaphore()
    for peer in (partner, right, left):
        pl.semaphore_signal(barrier, inc=1, device_id={"sp": peer}, device_id_type=MESH)
    pl.semaphore_wait(barrier, 3)

    def piece(src, half, peer, slot):
        return pltpu.make_async_remote_copy(
            src_ref=kv.at[src, half],
            dst_ref=kv.at[src, half],
            send_sem=send_sem.at[slot],
            recv_sem=recv_sem.at[src, half],
            device_id={"sp": peer},
            device_id_type=MESH,
        )

    own.wait()
    opp = rank(2, 0)
    sends = [
        piece(me, 0, right, 0), piece(me, 1, left, 1),
        piece(me, 0, partner, 2), piece(me, 1, partner, 3),
        piece(me, 1, right, 4), piece(me, 0, left, 5),
        piece(left, 0, right, 6), piece(right, 1, left, 7),
        piece(left, 0, partner, 8), piece(right, 1, partner, 9),
        piece(left, 1, partner, 10), piece(right, 0, partner, 11),
        piece(opp, 0, partner, 12), piece(opp, 1, partner, 13),
    ]
    for s in sends[:6]:
        s.start()

    m_s[...] = jnp.full(m_s.shape, NEG_BIG, jnp.float32)
    l_s[...] = jnp.zeros_like(l_s)
    acc_s[...] = jnp.zeros_like(acc_s)

    def update(a, src, b, gap, masked):
        for g in range(kv_loc):
            k_blk = kv[src, b, g * chunk:(g + 1) * chunk, :]
            base = kv_loc * chunk
            parts = [kv[src, b, base + (j * kv_loc + g) * head_dim:base + (j * kv_loc + g + 1) * head_dim, :] for j in range(chunk // 128)]
            v_t = jnp.concatenate(parts, axis=1)
            for t in range(tiles):
                s = lax.dot_general(k_blk, q_ref[a, g, t * TILE:(t + 1) * TILE, :], NT, preferred_element_type=jnp.float32)
                if masked:
                    low = (t * TILE) // chunk * chunk
                    base_col = t * TILE - low
                    raw = base_col + lax.broadcasted_iota(jnp.int32, (chunk, TILE), 1)
                    q_pos = jnp.where(raw >= chunk, raw - chunk, raw)
                    off = gap * chunk + q_pos - lax.broadcasted_iota(jnp.int32, (chunk, TILE), 0)
                    s = jnp.where((off >= 0) & (off < WINDOW), s, NEG_BIG)
                m_old = m_s[a, g, t]
                m_new = jnp.maximum(m_old, jnp.max(s, axis=0, keepdims=True))
                p = jnp.exp2((s - m_new) * scale)
                alpha = jnp.exp2((m_old - m_new) * scale)
                m_s[a, g, t] = m_new
                l_s[a, g, t] = l_s[a, g, t] * alpha + jnp.sum(p, axis=0, keepdims=True)
                acc_s[a, g, t] = acc_s[a, g, t] * alpha + lax.dot_general(v_t, p.astype(jnp.bfloat16), NN, preferred_element_type=jnp.float32)

    q_ids = (me, 2 * sp_size - 1 - me)
    order = [(0, 0, 0), (0, 0, 1), (0, 1, 0), (0, 1, 1), (-1, 0, 0), (1, 0, 1), (-1, 1, 0), (1, 1, 1),
             (-1, 0, 1), (1, 0, 0), (-1, 1, 1), (1, 1, 0), (2, 0, 0), (2, 0, 1), (2, 1, 0), (2, 1, 1)]
    forwards = {4: (6, 8), 5: (7, 9), 8: (10,), 9: (11,), 12: (12,), 13: (13,)}

    def pick(i, field):
        out = 0
        for n, entry in enumerate(order):
            if entry[field]:
                out = out + jnp.where(i == n, entry[field], 0)
        return out

    def item(i, carry):
        dx, flip, b = pick(i, 0), pick(i, 1), pick(i, 2)
        src_core = core + flip - 2 * core * flip
        src = 2 * lax.rem(chip + dx + chips, chips) + src_core

        @pl.when(i >= 2)
        def _():
            pltpu.make_async_remote_copy(
                src_ref=kv.at[src, b], dst_ref=kv.at[src, b], send_sem=send_sem.at[0], recv_sem=recv_sem.at[src, b],
                device_id={"sp": partner}, device_id_type=MESH).wait_recv()

        for n, slots in forwards.items():
            @pl.when(i == n)
            def _():
                for slot in slots:
                    sends[slot].start()

        k_id = b * (2 * sp_size - 1) + (1 - 2 * b) * src
        for a in range(2):
            gap = q_ids[a] - k_id
            needed = (gap >= 0) & (gap * chunk - chunk + 1 < WINDOW)
            masked = (gap == 0) | (gap * chunk + chunk - 1 >= WINDOW)

            @pl.when(needed & masked)
            def _():
                update(a, src, b, gap, True)

            @pl.when(needed & jnp.logical_not(masked))
            def _():
                update(a, src, b, gap, False)

        return carry

    lax.fori_loop(0, len(order), item, 0)

    for a in range(2):
        for g in range(kv_loc):
            norm = [acc_s[a, g, t] * (1.0 / l_s[a, g, t]) for t in range(tiles)]
            for t in range(tiles):
                for u in range(TILE // 128):
                    col = t * TILE + u * 128
                    h, row = g * group + col // chunk, col % chunk
                    o_ref[a * chunk + row:a * chunk + row + 128, h * head_dim:(h + 1) * head_dim] = norm[t][:, u * 128:(u + 1) * 128].T.astype(jnp.bfloat16)
    for s in sends:
        s.wait_send()


def attention(sp_size, q, kv):
    _, kv_loc, cols, head_dim = q.shape
    chunk = kv.shape[1] // (2 * kv_loc)
    group = cols // chunk
    tiles = cols // TILE
    return pl.pallas_call(
        functools.partial(attn_kernel, (sp_size, chunk, head_dim, kv_loc, group)),
        name="ring_attention",
        out_shape=jax.ShapeDtypeStruct((2 * chunk, kv_loc * group * head_dim), jnp.bfloat16),
        in_specs=[pl.BlockSpec(memory_space=pltpu.VMEM), pl.BlockSpec(memory_space=pl.ANY)],
        out_specs=pl.BlockSpec(memory_space=pltpu.VMEM),
        scratch_shapes=[
            pltpu.VMEM((sp_size,) + kv.shape, jnp.bfloat16),
            pltpu.VMEM((2, kv_loc, tiles, 1, TILE), jnp.float32),
            pltpu.VMEM((2, kv_loc, tiles, 1, TILE), jnp.float32),
            pltpu.VMEM((2, kv_loc, tiles, head_dim, TILE), jnp.float32),
            pltpu.SemaphoreType.DMA,
            pltpu.SemaphoreType.DMA((14,)),
            pltpu.SemaphoreType.DMA((sp_size, 2)),
        ],
        compiler_params=pltpu.CompilerParams(collective_id=1, has_side_effects=True, vmem_limit_bytes=56 << 20),
    )(q, kv)


def solution(mesh):
    sp_size = mesh.shape["sp"]

    def local_attn(x_part, w_query, w_key, w_value, w_out):
        x_block = lax.all_gather(x_part, "tp", axis=0, tiled=True)
        block_rows, d_model = x_block.shape
        chunk = block_rows // 2
        heads_loc, head_dim = w_query.shape[1], w_query.shape[2]
        kv_loc = w_key.shape[1]
        group = heads_loc // kv_loc

        def project(w):
            return jnp.dot(x_block, w.reshape(d_model, -1), preferred_element_type=jnp.float32).astype(jnp.bfloat16)

        q = project(w_query).reshape(2, chunk, kv_loc, group, head_dim).transpose(0, 2, 3, 1, 4).reshape(2, kv_loc, group * chunk, head_dim)
        k = project(w_key).reshape(2, chunk, kv_loc, head_dim).transpose(0, 2, 1, 3).reshape(2, kv_loc * chunk, head_dim)
        v = project(w_value).reshape(2, chunk // 128, 128, kv_loc, head_dim).transpose(0, 1, 3, 4, 2).reshape(2, kv_loc * chunk, 128)
        o = attention(sp_size, q, jnp.concatenate([k, v], axis=1))
        part_sum = jnp.dot(o, w_out.reshape(heads_loc * head_dim, d_model), preferred_element_type=jnp.float32)
        y_rows = lax.psum_scatter(part_sum, "tp", scatter_dimension=0, tiled=True)
        return y_rows.astype(jnp.bfloat16)

    return jax.shard_map(local_attn, mesh=mesh, in_specs=(P(("dp", "sp", "tp"), None), P(None, "tp", None), P(None, "tp", None), P(None, "tp", None), P("tp", None, None)), out_specs=P(("dp", "sp", "tp"), None), check_vma=False)
```

```python
import functools

import jax
import jax.numpy as jnp
from jax import lax
from jax.experimental import pallas as pl
from jax.experimental.pallas import tpu as pltpu
from jax.sharding import PartitionSpec as P

WINDOW = 4096
NEG_BIG = -1e30
LOG2E = 1.4426950408889634
TILE = 256
MESH = pl.DeviceIdType.MESH
NT = (((1,), (1,)), ((), ()))
NN = (((1,), (0,)), ((), ()))
ITEMS = [(dx, flip, b) for dx, flip in ((0, 0), (0, 1), (-1, 0), (1, 0), (-1, 1), (1, 1), (2, 0), (2, 1)) for b in (0, 1)]


def layer_kernel(dims, x_in, wq_in, wkv_in, wo_in, out, xs, wq, wkv, q_s, kv, m_s, l_s, acc_s, s_s, wo, o_s, ob, y_s,
                 load_sem, x_send, x_recv, kv_send, kv_recv, wo_load, wo_send, wo_recv, ob_send, ob_recv, y_send, y_recv, y_store):
    sp_size, tp_size, kv_loc, group, head_dim = dims
    chips = sp_size // 2
    rows, half = 2 * xs.shape[2], xs.shape[2]
    chunk = 2 * rows
    cols = group * chunk
    tiles = cols // TILE
    width = kv_loc * head_dim
    scale = head_dim ** -0.5 * LOG2E
    me, my_tp = lax.axis_index("sp"), lax.axis_index("tp")
    core, chip = lax.rem(me, 2), me // 2

    def rank(dx, flip):
        c = core if flip == 0 else 1 - core
        return 2 * lax.rem(chip + dx + chips, chips) + c

    partner, right, left, opp = rank(0, 1), rank(1, 0), rank(-1, 0), rank(2, 0)
    up, down, far = (lax.rem(my_tp + d, tp_size) for d in (1, tp_size - 1, 2))
    tps = (my_tp, down, up, far)

    loads = [pltpu.make_async_copy(x_in.at[pl.ds(h * half, half)], xs.at[0, h], load_sem.at[h]) for h in (0, 1)]
    loads += [pltpu.make_async_copy(wq_in, wq, load_sem.at[2]), pltpu.make_async_copy(wkv_in, wkv, load_sem.at[3])]
    for c in loads:
        c.start()
    w_rows, w_cols = wo.shape[3], wo.shape[4]

    def columns(quarter):
        return pl.ds(pl.multiple_of((core * chips + quarter) * w_cols, w_cols), w_cols)

    wo_loads = [pltpu.make_async_copy(wo_in.at[pl.ds(h * w_rows, w_rows), columns(lax.rem(chip + d, chips))],
                                      wo.at[my_tp, lax.rem(chip + d, chips), h], wo_load.at[d, h]) for d in range(chips) for h in (0, 1)]
    for c in wo_loads:
        c.start()
    barrier = pltpu.get_barrier_semaphore()
    peers = [{"sp": partner}, {"sp": right}, {"sp": left}, {"tp": up}, {"tp": down}, {"tp": far}]
    for peer in peers:
        pl.semaphore_signal(barrier, inc=1, device_id=peer, device_id_type=MESH)
    pl.semaphore_wait(barrier, len(peers))

    def x_piece(src, h, dst, peer, slot):
        return pltpu.make_async_remote_copy(
            src_ref=xs.at[src, h], dst_ref=xs.at[dst, h], send_sem=x_send.at[slot], recv_sem=x_recv.at[dst, h],
            device_id={"tp": peer}, device_id_type=MESH)

    x_sends = [x_piece(0, 0, 1, up, 0), x_piece(0, 1, 1, down, 1), x_piece(0, 1, 2, up, 2), x_piece(0, 0, 2, down, 3),
               x_piece(1, 0, 3, up, 4), x_piece(1, 1, 3, down, 5)]
    owners = ((my_tp, my_tp), (down, up), (up, down), (far, far))

    kv_sends = []

    def kv_copy(src, o, peer):
        copy = pltpu.make_async_remote_copy(
            src_ref=kv.at[src, tps[o]], dst_ref=kv.at[src, tps[o]], send_sem=kv_send.at[len(kv_sends)],
            recv_sem=kv_recv.at[src, tps[o]], device_id={"sp": peer}, device_id_type=MESH)
        kv_sends.append(copy)
        return copy

    own_kv = [[kv_copy(me, o, peer) for peer in (right, left, partner)] for o in range(4)]
    left_kv = [[kv_copy(left, o, peer) for peer in ((right, partner) if o < 2 else (partner,))] for o in range(4)]
    right_kv = [[kv_copy(right, o, peer) for peer in ((left, partner) if o >= 2 else (partner,))] for o in range(4)]
    opp_kv = [[kv_copy(opp, o, partner)] for o in range(4)]

    def start(copies):
        for c in copies:
            c.start()

    def kv_wait(src, o):
        pltpu.make_async_remote_copy(
            src_ref=kv.at[src, tps[o]], dst_ref=kv.at[src, tps[o]], send_sem=kv_send.at[0], recv_sem=kv_recv.at[src, tps[o]],
            device_id={"sp": partner}, device_id_type=MESH).wait_recv()

    def pass_on(side, src, orders):
        for o in orders:
            kv_wait(src, o)
            start(side[o])

    wo_sends = []

    def wo_copy(o, dx, h, peer):
        at = (tps[o], lax.rem(chip + dx + chips, chips), h)
        copy = pltpu.make_async_remote_copy(
            src_ref=wo.at[at], dst_ref=wo.at[at], send_sem=wo_send.at[len(wo_sends)], recv_sem=wo_recv.at[at],
            device_id=peer, device_id_type=MESH)
        wo_sends.append(copy)
        return copy

    def wo_wait(o, dx, h):
        at = (tps[o], lax.rem(chip + dx + chips, chips), h)
        pltpu.make_async_remote_copy(
            src_ref=wo.at[at], dst_ref=wo.at[at], send_sem=wo_send.at[0], recv_sem=wo_recv.at[at],
            device_id={"sp": partner}, device_id_type=MESH).wait_recv()

    to_up, to_down, to_right, to_left = {"tp": up}, {"tp": down}, {"sp": right}, {"sp": left}
    wo_first = [wo_copy(0, 0, 0, to_up), wo_copy(0, 0, 1, to_down)]
    wo_second = [wo_copy(0, 0, 1, to_up), wo_copy(0, 0, 0, to_down)]
    wo_third = [wo_copy(1, 0, 0, to_up), wo_copy(2, 0, 1, to_down)]
    wo_side = {(o, h): [wo_copy(o, 0, h, to_right), wo_copy(o, 0, h, to_left)] for o in (1, 2, 3) for h in (0, 1)}
    wo_relay = {o: [wo_copy(o, -1, 0, to_right), wo_copy(o, 1, 1, to_left)] for o in (1, 2, 3)}

    def relay(o):
        wo_wait(o, -1, 0)
        wo_relay[o][0].start()
        wo_wait(o, 1, 1)
        wo_relay[o][1].start()

    def project(step):
        x_rows = xs[step].reshape(rows, xs.shape[3])
        kv_rows = jnp.dot(x_rows, wkv[...], preferred_element_type=jnp.float32).astype(jnp.bfloat16)
        for h in (0, 1):
            kv[me, owners[step][h], h * half:(h + 1) * half, :] = kv_rows[h * half:(h + 1) * half]
        for g in range(kv_loc):
            for hh in range(group):
                if hh % 2:
                    continue
                lane = (g * group + hh) * head_dim
                res = jnp.dot(x_rows, wq[:, lane:lane + 2 * head_dim], preferred_element_type=jnp.float32).astype(jnp.bfloat16)
                for h in (0, 1):
                    tp = owners[step][h]
                    for n in (0, 1):
                        base = pl.multiple_of((hh + n) * chunk + lax.rem(tp, 2) * rows + h * half, half)
                        q_s[tp // 2, g, pl.ds(base, half), :] = res[h * half:(h + 1) * half, n * head_dim:(n + 1) * head_dim]

    loads[0].wait()
    loads[1].wait()
    for c in wo_loads[:2]:
        c.wait()
    start(wo_first)
    start(x_sends[:4])
    m_s[...] = jnp.full(m_s.shape, NEG_BIG, jnp.float32)
    l_s[...] = jnp.zeros_like(l_s)
    acc_s[...] = jnp.zeros_like(acc_s)
    loads[2].wait()
    loads[3].wait()
    def steps(step, carry):
        @pl.when(step == 1)
        def _():
            start(own_kv[0])
            for o, h in ((1, 0), (2, 1)):
                wo_wait(o, 0, h)
                start(wo_side[o, h])
            x_sends[0].wait_recv()
            x_sends[4].start()
            x_sends[1].wait_recv()
            x_sends[5].start()
            start(wo_second)
            start(wo_third)
            pass_on(left_kv, left, (0,))
            pass_on(right_kv, right, (0,))

        @pl.when(step == 2)
        def _():
            x_sends[2].wait_recv()
            x_sends[3].wait_recv()
            pass_on(opp_kv, opp, (0,))
            wo_wait(1, -1, 0)
            wo_relay[1][0].start()
            wo_wait(2, 1, 1)
            wo_relay[2][1].start()

        @pl.when(step == 3)
        def _():
            start(own_kv[1])
            start(own_kv[2])
            x_sends[4].wait_recv()
            x_sends[5].wait_recv()
            pass_on(left_kv, left, (1, 2))
            pass_on(right_kv, right, (1, 2))

        for n in range(4):
            @pl.when(step == n)
            def _():
                project(n)
        return carry

    lax.fori_loop(0, 4, steps, 0)
    start(own_kv[3])

    def update(a, src, b, gap, masked):
        todo = [(g, t) for g in range(kv_loc) for t in range(tiles)]

        def block(lane):
            return kv[src, pl.ds(2 * b, 2), :, lane:lane + head_dim].reshape(chunk, head_dim)

        def scores(n):
            g, t = todo[n]
            s_s[n % 2] = lax.dot_general(block(g * head_dim), q_s[a, g, t * TILE:(t + 1) * TILE, :], NT, preferred_element_type=jnp.float32)

        scores(0)
        v_t = [block(width + g * head_dim).T for g in range(kv_loc)]
        for n, (g, t) in enumerate(todo):
            if n + 1 < len(todo):
                scores(n + 1)
            s = s_s[n % 2]
            if masked:
                raw = t * TILE % chunk + lax.broadcasted_iota(jnp.int32, (chunk, TILE), 1)
                q_pos = jnp.where(raw >= chunk, raw - chunk, raw)
                off = gap * chunk + q_pos - lax.broadcasted_iota(jnp.int32, (chunk, TILE), 0)
                s = jnp.where((off >= 0) & (off < WINDOW), s, NEG_BIG)
            m_old = m_s[a, g, t]
            m_new = jnp.maximum(m_old, jnp.max(s, axis=0, keepdims=True))
            p = jnp.exp2((s - m_new) * scale)
            alpha = jnp.exp2((m_old - m_new) * scale)
            m_s[a, g, t] = m_new
            l_s[a, g, t] = l_s[a, g, t] * alpha + jnp.sum(p, axis=0, keepdims=True)
            acc_s[a, g, t] = acc_s[a, g, t] * alpha + lax.dot_general(v_t[g], p.astype(jnp.bfloat16), NN, preferred_element_type=jnp.float32)

    def wait_all(src):
        for o in range(4):
            kv_wait(src, o)

    def before(i):
        @pl.when(i == 2)
        def _():
            wait_all(partner)
            pass_on(opp_kv, opp, (1, 2))

        @pl.when(i == 4)
        def _():
            pass_on(left_kv, left, (3,))
            pass_on(right_kv, right, (3,))

        @pl.when(i == 8)
        def _():
            wait_all(rank(-1, 1))
            wait_all(rank(1, 1))
            pass_on(opp_kv, opp, (3,))
            for o, h in ((1, 1), (2, 0)):
                wo_wait(o, 0, h)
                start(wo_side[o, h])

        @pl.when(i == 12)
        def _():
            for h in (0, 1):
                wo_wait(3, 0, h)
                start(wo_side[3, h])

        @pl.when(i == 14)
        def _():
            wait_all(rank(2, 1))

    def pick(i, field):
        out = 0
        for n, entry in enumerate(ITEMS):
            if entry[field]:
                out = out + jnp.where(i == n, entry[field], 0)
        return out

    q_ids = (me, 2 * sp_size - 1 - me)

    def item(i, carry):
        before(i)
        dx, flip, b = pick(i, 0), pick(i, 1), pick(i, 2)
        src = 2 * lax.rem(chip + dx + chips, chips) + core + flip - 2 * core * flip
        k_id = b * (2 * sp_size - 1) + (1 - 2 * b) * src
        for a in range(2):
            gap = q_ids[a] - k_id
            needed = (gap >= 0) & (gap * chunk - chunk + 1 < WINDOW)
            masked = (gap == 0) | (gap * chunk + chunk - 1 >= WINDOW)

            @pl.when(needed & masked)
            def _():
                update(a, src, b, gap, True)

            @pl.when(needed & jnp.logical_not(masked))
            def _():
                update(a, src, b, gap, False)

        return carry

    lax.fori_loop(0, len(ITEMS), item, 0)

    for a in range(2):
        for g in range(kv_loc):
            for t in range(tiles):
                norm = acc_s[a, g, t] * (1.0 / l_s[a, g, t])
                for u in range(TILE // 64):
                    col = t * TILE + u * 64
                    h, row = g * group + col // chunk, col % chunk
                    if u % 2 == 0:
                        turned = norm[:, u * 64:u * 64 + 128].T.astype(jnp.bfloat16)
                    o_s[2 * a + row // rows, row % rows:row % rows + 64, h * head_dim:(h + 1) * head_dim] = turned[u % 2 * 64:u % 2 * 64 + 64]

    ob_sends = []

    def ob_copy(src, o, peer):
        copy = pltpu.make_async_remote_copy(
            src_ref=src, dst_ref=ob.at[tps[o], core], send_sem=ob_send.at[len(ob_sends)], recv_sem=ob_recv.at[tps[o], core],
            device_id=peer, device_id_type=MESH)
        ob_sends.append(copy)
        return copy

    ob[my_tp, core] = o_s[my_tp]
    start([ob_copy(o_s.at[tps[o]], 0, {"tp": tps[o]}) for o in (3, 1, 2)])
    start([ob_copy(ob.at[my_tp, core], 0, {"sp": partner})])

    def ob_wait(o, c):
        at = (tps[o], c)
        pltpu.make_async_remote_copy(
            src_ref=ob.at[at], dst_ref=ob.at[at], send_sem=ob_send.at[0], recv_sem=ob_recv.at[at],
            device_id={"sp": partner}, device_id_type=MESH).wait_recv()

    wo_wait(2, -1, 0)
    wo_relay[2][0].start()
    wo_wait(1, 1, 1)
    wo_relay[1][1].start()
    for o in (1, 2, 3):
        ob_wait(o, core)
        start([ob_copy(ob.at[tps[o], core], o, {"sp": partner})])
    for o in range(4):
        ob_wait(o, 1 - core)
    for c in wo_loads[2:]:
        c.wait()

    def y_remote(n, quarter):
        return pltpu.make_async_remote_copy(
            src_ref=y_s.at[n, 1 - core], dst_ref=out.at[:, columns(quarter)], send_sem=y_send.at[n], recv_sem=y_recv.at[n],
            device_id={"sp": partner}, device_id_type=MESH)

    def y_local(n, quarter):
        return pltpu.make_async_copy(y_s.at[n, core], out.at[:, columns(quarter)], y_store.at[n])

    def quarter_of(n):
        return lax.rem(chip + jnp.where(n == 1, chips - 1, jnp.where(n == 2, 1, jnp.where(n == 3, 2, 0))), chips)

    def finish(n, carry):
        @pl.when(n == 1)
        def _():
            relay(3)
            wo_wait(1, -1, 1)
            wo_wait(2, -1, 1)
            wo_wait(3, -1, 1)

        @pl.when(n == 2)
        def _():
            for o in (1, 2, 3):
                wo_wait(o, 1, 0)

        @pl.when(n == 3)
        def _():
            for o in (1, 2, 3):
                for h in (0, 1):
                    wo_wait(o, 2, h)

        quarter = quarter_of(n)
        for part in range(0, w_cols, TILE):
            total = None
            for tp in range(tp_size):
                res = jnp.dot(ob[tp].reshape(2 * rows, 2 * w_rows), wo[tp, quarter, :, :, part:part + TILE].reshape(2 * w_rows, TILE),
                              preferred_element_type=jnp.float32)
                total = res if total is None else total + res
            y_s[n, :, :, part:part + TILE] = total.astype(jnp.bfloat16).reshape(2, rows, TILE)
        y_remote(n, quarter).start()
        y_local(n, quarter).start()
        return carry

    lax.fori_loop(0, chips, finish, 0)
    for n in range(chips):
        y_remote(n, quarter_of(n)).wait()
        y_local(n, quarter_of(n)).wait()
    for c in x_sends + kv_sends + wo_sends + ob_sends:
        c.wait_send()


def layer(sp_size, tp_size, heads, x_part, w_q, w_kv, w_o):
    kv_loc, group, head_dim = heads
    rows, d_model = x_part.shape
    chunk = 2 * rows
    tiles = group * chunk // TILE
    width = kv_loc * head_dim
    chips = sp_size // 2
    quarter = d_model // sp_size
    f32, bf16 = jnp.float32, jnp.bfloat16
    dma = pltpu.SemaphoreType.DMA
    return pl.pallas_call(
        functools.partial(layer_kernel, (sp_size, tp_size) + heads),
        name="layer",
        out_shape=jax.ShapeDtypeStruct(x_part.shape, bf16),
        in_specs=[pl.BlockSpec(memory_space=pl.ANY)] * 4,
        out_specs=pl.BlockSpec(memory_space=pl.ANY),
        scratch_shapes=[
            pltpu.VMEM((4, 2, rows // 2, d_model), bf16),
            pltpu.VMEM(w_q.shape, bf16),
            pltpu.VMEM(w_kv.shape, bf16),
            pltpu.VMEM((2, kv_loc, group * chunk, head_dim), bf16),
            pltpu.VMEM((sp_size, tp_size, rows, 2 * width), bf16),
            pltpu.VMEM((2, kv_loc, tiles, 1, TILE), f32),
            pltpu.VMEM((2, kv_loc, tiles, 1, TILE), f32),
            pltpu.VMEM((2, kv_loc, tiles, head_dim, TILE), f32),
            pltpu.VMEM((2, chunk, TILE), f32),
            pltpu.VMEM((tp_size, chips, 2, w_o.shape[0] // 2, quarter), bf16),
            pltpu.VMEM((tp_size, rows, w_o.shape[0]), bf16),
            pltpu.VMEM((tp_size, 2, rows, w_o.shape[0]), bf16),
            pltpu.VMEM((chips, 2, rows, quarter), bf16),
            dma((4,)), dma((6,)), dma((4, 2)), dma((28,)), dma((sp_size, tp_size)),
            dma((chips, 2)), dma((24,)), dma((tp_size, chips, 2)), dma((7,)), dma((tp_size, 2)), dma((chips,)), dma((chips,)), dma((chips,)),
        ],
        compiler_params=pltpu.CompilerParams(collective_id=1, has_side_effects=True, vmem_limit_bytes=62 << 20),
    )(x_part, w_q, w_kv, w_o)


def solution(mesh):
    sp_size, tp_size = mesh.shape["sp"], mesh.shape["tp"]

    def local_attn(x_part, w_query, w_key, w_value, w_out):
        d_model = x_part.shape[1]
        heads_loc, head_dim = w_query.shape[1], w_query.shape[2]
        kv_loc = w_key.shape[1]
        w_q = w_query.reshape(d_model, -1)
        w_kv = jnp.concatenate([w_key.reshape(d_model, -1), w_value.reshape(d_model, -1)], axis=1)
        w_o = w_out.reshape(-1, d_model)
        return layer(sp_size, tp_size, (kv_loc, heads_loc // kv_loc, head_dim), x_part, w_q, w_kv, w_o)

    return jax.shard_map(local_attn, mesh=mesh, in_specs=(P(("dp", "sp", "tp"), None), P(None, "tp", None), P(None, "tp", None), P(None, "tp", None), P("tp", None, None)), out_specs=P(("dp", "sp", "tp"), None), check_vma=False)
```

```python
import functools

import jax
import jax.numpy as jnp
from jax import lax
from jax.experimental import pallas as pl
from jax.experimental.pallas import tpu as pltpu
from jax.sharding import PartitionSpec as P

WINDOW = 4096
NEG_BIG = -1e30
LOG2E = 1.4426950408889634
TILE = 768
WEIGHT_ROWS = 512
MESH = pl.DeviceIdType.MESH
NT = (((1,), (1,)), ((), ()))
NN = (((1,), (0,)), ((), ()))
SUBS = 4
SECOND_EARLY = True
WEIGHT_EVENTS = [(3, ((1, 3), (2, 0))), (4, ((3, 0), (3, 3))), (7, ((3, 1), (3, 2)))] if SECOND_EARLY else [
    (5, ((1, 2), (2, 1))), (7, ((1, 3), (2, 0))), (9, ((3, 0), (3, 3))), (12, ((3, 1), (3, 2)))]
ITEMS = [(dx, flip, f) for group in ([(0, 0)], [(0, 1)], [(-1, 0), (1, 0)], [(-1, 1), (1, 1)], [(2, 0)], [(2, 1)]) for f in (0, 1) for dx, flip in group]


def layer_kernel(dims, x_in, wq_in, wk_in, wv_in, wo_in, out, raw_q, raw_k, raw_v, xs, wq, wkv, q_s, kv, m_s, l_s, acc_s, s_s, wo, o_s, ob, via, total_s, y_s,
                 load_sem, raw_sem, x_send, x_recv, kv_send, kv_recv, wo_load, wo_send, wo_recv, ob_send, ob_recv, via_recv, far_recv, y_send, y_recv, y_store):
    sp_size, tp_size, kv_loc, group, head_dim = dims
    chips = sp_size // 2
    rows, half = 2 * xs.shape[2], xs.shape[2]
    chunk = 2 * rows
    cols = group * chunk
    tiles = cols // TILE
    width = kv_loc * head_dim
    scale = head_dim ** -0.5 * LOG2E
    me, my_tp = lax.axis_index("sp"), lax.axis_index("tp")
    core, chip = lax.rem(me, 2), me // 2

    def rank(dx, flip):
        c = core if flip == 0 else 1 - core
        return 2 * lax.rem(chip + dx + chips, chips) + c

    partner, right, left, opp = rank(0, 1), rank(1, 0), rank(-1, 0), rank(2, 0)
    up, down, far = (lax.rem(my_tp + d, tp_size) for d in (1, tp_size - 1, 2))
    tps = (my_tp, down, up, far)

    barrier = pltpu.get_barrier_semaphore()
    peers = [{"sp": partner}, {"sp": right}, {"sp": left}, {"tp": up}, {"tp": down}]
    for peer in peers:
        pl.semaphore_signal(barrier, inc=1, device_id=peer, device_id_type=MESH)
    loads = [pltpu.make_async_copy(x_in.at[pl.ds(h * half, half)], xs.at[0, h], load_sem.at[h]) for h in (0, 1)]
    for c in loads:
        c.start()
    step_rows = raw_q.shape[1]
    w_chunks = xs.shape[3] // step_rows
    raw = ((wq_in, raw_q, wq, 0), (wk_in, raw_k, wkv, 0), (wv_in, raw_v, wkv, width))

    def raw_load(n, k):
        return pltpu.make_async_copy(raw[k][0].at[pl.ds(pl.multiple_of(n * step_rows, step_rows), step_rows)], raw[k][1].at[lax.rem(n, 2)], raw_sem.at[lax.rem(n, 2), k])

    def flatten_weights():
        def body(n, carry):
            rows_n = pl.ds(pl.multiple_of(n * step_rows, step_rows), step_rows)
            for k, (_, src, dst, lane) in enumerate(raw):
                raw_load(n, k).wait()
                flat = src[lax.rem(n, 2)].reshape(step_rows, src.shape[2] * src.shape[3])
                dst[rows_n, lane:lane + flat.shape[1]] = flat

                @pl.when(n + 2 < w_chunks)
                def _():
                    raw_load(n + 2, k).start()
            return carry

        lax.fori_loop(0, w_chunks, body, 0)

    for n in (0, 1):
        for k in range(3):
            raw_load(n, k).start()
    w_rows, w_cols = wo.shape[3], wo.shape[4]

    def columns(quarter):
        return pl.ds(pl.multiple_of((core * chips + quarter) * w_cols, w_cols), w_cols)

    wo_loads = [pltpu.make_async_copy(wo_in.at[pl.ds(h * w_rows, w_rows), columns(lax.rem(chip + d, chips))],
                                      wo.at[my_tp, lax.rem(chip + d, chips), h], wo_load.at[d, h]) for d in range(chips) for h in range(SUBS)]
    for c in wo_loads:
        c.start()
    pl.semaphore_wait(barrier, len(peers))

    def x_piece(src, h, dst, peer, slot):
        return pltpu.make_async_remote_copy(
            src_ref=xs.at[src, h], dst_ref=xs.at[dst, h], send_sem=x_send.at[slot], recv_sem=x_recv.at[dst, h],
            device_id={"tp": peer}, device_id_type=MESH)

    x_sends = [x_piece(0, 0, 1, up, 0), x_piece(0, 1, 1, down, 1), x_piece(0, 1, 2, up, 2), x_piece(0, 0, 2, down, 3),
               x_piece(1, 0, 3, up, 4), x_piece(1, 1, 3, down, 5)]
    owners = ((my_tp, my_tp), (down, up), (up, down), (far, far))

    kv_sends = []

    def kv_copy(src, o, peer):
        copy = pltpu.make_async_remote_copy(
            src_ref=kv.at[src, tps[o]], dst_ref=kv.at[src, tps[o]], send_sem=kv_send.at[len(kv_sends)],
            recv_sem=kv_recv.at[src, tps[o]], device_id={"sp": peer}, device_id_type=MESH)
        kv_sends.append(copy)
        return copy

    own_kv = [[kv_copy(me, o, peer) for peer in (right, left, partner)] for o in range(4)]
    left_kv = [[kv_copy(left, o, peer) for peer in ((right, partner) if o < 2 else (partner,))] for o in range(4)]
    right_kv = [[kv_copy(right, o, peer) for peer in ((left, partner) if o >= 2 else (partner,))] for o in range(4)]
    opp_kv = [[kv_copy(opp, o, partner)] for o in range(4)]

    def start(copies):
        for c in copies:
            c.start()

    def kv_wait(src, o):
        pltpu.make_async_remote_copy(
            src_ref=kv.at[src, tps[o]], dst_ref=kv.at[src, tps[o]], send_sem=kv_send.at[0], recv_sem=kv_recv.at[src, tps[o]],
            device_id={"sp": partner}, device_id_type=MESH).wait_recv()

    def pass_on(side, src, orders):
        for o in orders:
            kv_wait(src, o)
            start(side[o])

    wo_sends = []

    def wo_copy(o, dx, h, peer):
        at = (tps[o], lax.rem(chip + dx + chips, chips), h)
        copy = pltpu.make_async_remote_copy(
            src_ref=wo.at[at], dst_ref=wo.at[at], send_sem=wo_send.at[len(wo_sends)], recv_sem=wo_recv.at[at],
            device_id=peer, device_id_type=MESH)
        wo_sends.append(copy)
        return copy

    def wo_wait(o, dx, h):
        at = (tps[o], lax.rem(chip + dx + chips, chips), h)
        pltpu.make_async_remote_copy(
            src_ref=wo.at[at], dst_ref=wo.at[at], send_sem=wo_send.at[0], recv_sem=wo_recv.at[at],
            device_id={"sp": partner}, device_id_type=MESH).wait_recv()

    to_up, to_down, to_right, to_left = {"tp": up}, {"tp": down}, {"sp": right}, {"sp": left}
    def both_ways(pairs):
        return [c for h in pairs for c in (wo_copy(0, 0, h, to_up), wo_copy(0, 0, SUBS - 1 - h, to_down))]

    wo_first = both_ways((0, 1))
    wo_second = both_ways((2, 3))
    wo_third = [c for h in (0, 1) for c in (wo_copy(1, 0, h, to_up), wo_copy(2, 0, SUBS - 1 - h, to_down))]
    wo_side = {(o, h): [wo_copy(o, 0, h, to_right), wo_copy(o, 0, h, to_left)] for o in (1, 2, 3) for h in range(SUBS)}
    wo_relay = {(o, h): wo_copy(o, -1 if h < SUBS // 2 else 1, h, to_right if h < SUBS // 2 else to_left)
                for o, subs in ((1, (0, 1)), (2, (3, 2)), (3, (0, 3, 1, 2))) for h in subs}
    wo_last = [c for h in (0, 1) for c in (wo_copy(0, 2, SUBS // 2 + h, to_up), wo_copy(0, 2, h, to_down))]

    def spread(o, h):
        wo_wait(o, 0, h)
        start(wo_side[o, h])

    def relay(o, h):
        wo_wait(o, -1 if h < SUBS // 2 else 1, h)
        wo_relay[o, h].start()

    def project(step):
        x_rows = xs[step].reshape(rows, xs.shape[3])
        kv_rows = jnp.dot(x_rows, wkv[...], preferred_element_type=jnp.float32).astype(jnp.bfloat16)
        for h in (0, 1):
            kv[me, owners[step][h], h * half:(h + 1) * half, :] = kv_rows[h * half:(h + 1) * half]
        for g in range(kv_loc):
            for hh in range(group):
                if hh % 2:
                    continue
                lane = (g * group + hh) * head_dim
                res = jnp.dot(x_rows, wq[:, lane:lane + 2 * head_dim], preferred_element_type=jnp.float32).astype(jnp.bfloat16)
                for h in (0, 1):
                    tp = owners[step][h]
                    for n in (0, 1):
                        base = pl.multiple_of((hh + n) * chunk + lax.rem(tp, 2) * rows + h * half, half)
                        q_s[tp // 2, g, pl.ds(base, half), :] = res[h * half:(h + 1) * half, n * head_dim:(n + 1) * head_dim]

    loads[0].wait()
    loads[1].wait()
    for c in wo_loads[:SUBS]:
        c.wait()
    start(wo_first)
    start(x_sends[:4])
    if SECOND_EARLY:
        start(wo_second[:2])
    m_s[...] = jnp.full(m_s.shape, NEG_BIG, jnp.float32)
    l_s[...] = jnp.zeros_like(l_s)
    acc_s[...] = jnp.zeros_like(acc_s)
    flatten_weights()
    def steps(step, carry):
        @pl.when(step == 1)
        def _():
            start(own_kv[0])
            for o, h in ((1, 0), (2, 3), (1, 1), (2, 2)):
                spread(o, h)
            x_sends[0].wait_recv()
            x_sends[4].start()
            x_sends[1].wait_recv()
            x_sends[5].start()
            start(wo_second[2 if SECOND_EARLY else 0:])
            start(wo_third)
            pass_on(left_kv, left, (0,))
            pass_on(right_kv, right, (0,))
            for c in wo_loads[SUBS:]:
                c.wait()

        @pl.when(step == 2)
        def _():
            for o, h in ((1, 0), (2, 3), (1, 1), (2, 2)):
                relay(o, h)
            x_sends[2].wait_recv()
            x_sends[3].wait_recv()

        @pl.when(step == 3)
        def _():
            start(own_kv[1])
            start(own_kv[2])
            pass_on(opp_kv, opp, (0,))
            if SECOND_EARLY:
                spread(1, 2)
                spread(2, 1)
            x_sends[4].wait_recv()
            x_sends[5].wait_recv()

        for n in range(4):
            @pl.when(step == n)
            def _():
                project(n)
        return carry

    lax.fori_loop(0, 4, steps, 0)
    start(own_kv[3])

    def update(a, src, b, gap, masked):
        todo = [(g, t) for g in range(kv_loc) for t in range(tiles)]

        def block(lane):
            return kv[src, pl.ds(2 * b, 2), :, lane:lane + head_dim].reshape(chunk, head_dim)

        def scores(n):
            g, t = todo[n]
            s_s[n % 2] = lax.dot_general(block(g * head_dim), q_s[a, g, t * TILE:(t + 1) * TILE, :], NT, preferred_element_type=jnp.float32)

        scores(0)
        v_t = [block(width + g * head_dim).T for g in range(kv_loc)]
        for n, (g, t) in enumerate(todo):
            if n + 1 < len(todo):
                scores(n + 1)
            s = s_s[n % 2]
            if masked:
                raw = t * TILE % chunk + lax.broadcasted_iota(jnp.int32, (chunk, TILE), 1)
                q_pos = jnp.where(raw >= chunk, raw - chunk, raw)
                off = gap * chunk + q_pos - lax.broadcasted_iota(jnp.int32, (chunk, TILE), 0)
                s = jnp.where((off >= 0) & (off < WINDOW), s, NEG_BIG)
            m_old = m_s[a, g, t]
            m_new = jnp.maximum(m_old, jnp.max(s, axis=0, keepdims=True))
            p = jnp.exp2((s - m_new) * scale)
            alpha = jnp.exp2((m_old - m_new) * scale)
            m_s[a, g, t] = m_new
            l_s[a, g, t] = l_s[a, g, t] * alpha + jnp.sum(p, axis=0, keepdims=True)
            acc_s[a, g, t] = acc_s[a, g, t] * alpha + lax.dot_general(v_t[g], p.astype(jnp.bfloat16), NN, preferred_element_type=jnp.float32)

    def wait_for(src, orders):
        for o in orders:
            kv_wait(src, o)

    def before(i, past, done):
        near = (0, 1, 2)

        @pl.when((past < 3) & (done >= 3))
        def _():
            pass_on(left_kv, left, (3,))
            pass_on(right_kv, right, (3,))

        for threshold, pieces in WEIGHT_EVENTS:
            @pl.when((past < threshold) & (done >= threshold))
            def _():
                for o, h in pieces:
                    if o == 3:
                        wo_wait(o, 0, h)
                    else:
                        spread(o, h)
                if pieces[0][0] == 3:
                    first, last = (wo_side[piece] for piece in pieces)
                    start([first[0], last[1], last[0], first[1]])

        @pl.when(i == 0)
        def _():
            pass_on(left_kv, left, (1, 2))
            pass_on(right_kv, right, (1, 2))
            start(wo_last)

        @pl.when(i == 2)
        def _():
            wait_for(partner, near)

        @pl.when(i == 3)
        def _():
            wait_for(partner, (3,))

        @pl.when(i == 8)
        def _():
            wait_for(rank(-1, 1), near)
            wait_for(rank(1, 1), near)
            pass_on(opp_kv, opp, (1, 2))

        @pl.when(i == 10)
        def _():
            wait_for(rank(-1, 1), (3,))
            wait_for(rank(1, 1), (3,))
            pass_on(opp_kv, opp, (3,))

        @pl.when(i == 14)
        def _():
            wait_for(rank(2, 1), near)

        @pl.when(i == 15)
        def _():
            wait_for(rank(2, 1), (3,))

    def pick(i, field):
        out = 0
        for n, entry in enumerate(ITEMS):
            if entry[field]:
                out = out + jnp.where(i == n, entry[field], 0)
        return out

    q_ids = (me, 2 * sp_size - 1 - me)

    def item(i, carry):
        past, done = carry
        before(i, past, done)
        past = done
        dx, flip, f = pick(i, 0), pick(i, 1), pick(i, 2)
        own_b = my_tp // 2
        b = own_b + f - 2 * own_b * f
        src = 2 * lax.rem(chip + dx + chips, chips) + core + flip - 2 * core * flip
        k_id = b * (2 * sp_size - 1) + (1 - 2 * b) * src
        for a in range(2):
            gap = q_ids[a] - k_id
            needed = (gap >= 0) & (gap * chunk - chunk + 1 < WINDOW)
            masked = (gap == 0) | (gap * chunk + chunk - 1 >= WINDOW)
            done = done + needed.astype(jnp.int32)

            @pl.when(needed & masked)
            def _():
                update(a, src, b, gap, True)

            @pl.when(needed & jnp.logical_not(masked))
            def _():
                update(a, src, b, gap, False)

        return past, done

    lax.fori_loop(0, len(ITEMS), item, (0, 0))

    for a in range(2):
        for g in range(kv_loc):
            for t in range(tiles):
                norm = acc_s[a, g, t] * (1.0 / l_s[a, g, t])
                for u in range(TILE // 64):
                    col = t * TILE + u * 64
                    h, row = g * group + col // chunk, col % chunk
                    if u % 2 == 0:
                        turned = norm[:, u * 64:u * 64 + 128].T.astype(jnp.bfloat16)
                    o_s[2 * a + row // rows, row % rows:row % rows + 64, h * head_dim:(h + 1) * head_dim] = turned[u % 2 * 64:u % 2 * 64 + 64]

    ob_sends = []

    def ob_copy(src, dst, recv, peer):
        copy = pltpu.make_async_remote_copy(
            src_ref=src, dst_ref=dst, send_sem=ob_send.at[len(ob_sends)], recv_sem=recv, device_id=peer, device_id_type=MESH)
        ob_sends.append(copy)
        return copy

    def ob_wait(ref, recv):
        pltpu.make_async_remote_copy(
            src_ref=ref, dst_ref=ref, send_sem=ob_send.at[0], recv_sem=recv, device_id={"sp": partner}, device_id_type=MESH).wait_recv()

    def part(h):
        return pl.ds(h * half, half)

    ob[my_tp, core] = o_s[my_tp]
    start([ob_copy(o_s.at[far, part(0)], via.at[0], via_recv.at[0], to_up), ob_copy(o_s.at[far, part(1)], via.at[1], via_recv.at[1], to_down)])
    start([ob_copy(o_s.at[up], ob.at[my_tp, core], ob_recv.at[my_tp, 0], to_up), ob_copy(o_s.at[down], ob.at[my_tp, core], ob_recv.at[my_tp, 0], to_down)])
    start([ob_copy(ob.at[my_tp, core], ob.at[my_tp, core], ob_recv.at[my_tp, 1], {"sp": partner})])
    def share(source, quarter):
        return jnp.dot(ob[source].reshape(2 * rows, SUBS * w_rows), wo[source, quarter].reshape(SUBS * w_rows, w_cols), preferred_element_type=jnp.float32)

    def quarter_of(n):
        return lax.rem(chip + jnp.where(n == 1, chips - 1, jnp.where(n == 2, 1, jnp.where(n == 3, 2, 0))), chips)

    def gather_own(n, carry):
        total_s[n] = share(my_tp, quarter_of(n))
        return carry

    for h, source, peer in ((0, down, to_up), (1, up, to_down)):
        ob_wait(via.at[h], via_recv.at[h])
        start([ob_copy(via.at[h], ob.at[source, core, part(h)], far_recv.at[h], peer)])
    for h in (0, 3, 1, 2):
        relay(3, h)
    ob_wait(ob.at[my_tp, 1 - core], ob_recv.at[my_tp, 1])
    lax.fori_loop(0, chips, gather_own, 0)
    for source in (down, up):
        ob_wait(ob.at[source, core], ob_recv.at[source, 0])
        start([ob_copy(ob.at[source, core], ob.at[source, core], ob_recv.at[source, 1], {"sp": partner})])
    far_share = ob_copy(ob.at[far, core], ob.at[far, core], ob_recv.at[far, 1], {"sp": partner})
    for source in (down, up):
        ob_wait(ob.at[source, 1 - core], ob_recv.at[source, 1])

    def y_remote(n, quarter):
        return pltpu.make_async_remote_copy(
            src_ref=y_s.at[n, 1 - core], dst_ref=out.at[:, columns(quarter)], send_sem=y_send.at[n], recv_sem=y_recv.at[n],
            device_id={"sp": partner}, device_id_type=MESH)

    def y_local(n, quarter):
        return pltpu.make_async_copy(y_s.at[n, core], out.at[:, columns(quarter)], y_store.at[n])

    def gather_near(n, carry):
        @pl.when(n == 1)
        def _():
            for h in (0, 1):
                ob_wait(ob.at[far, core, part(h)], far_recv.at[h])
            far_share.start()
            for o, h in ((1, 2), (1, 3), (2, 0), (2, 1), (2, 2), (2, 3), (3, 2), (3, 3)):
                wo_wait(o, -1, h)

        @pl.when(n == 2)
        def _():
            for o, h in ((1, 0), (1, 1), (1, 2), (1, 3), (2, 0), (2, 1), (3, 0), (3, 1)):
                wo_wait(o, 1, h)

        @pl.when(n == 3)
        def _():
            for o in (1, 2, 3):
                for h in range(SUBS):
                    wo_wait(o, 2, h)

        quarter = quarter_of(n)
        total_s[n] = total_s[n] + share(down, quarter) + share(up, quarter)
        return carry

    def finish(n, carry):
        quarter = quarter_of(n)
        y_s[n] = (total_s[n] + share(far, quarter)).astype(jnp.bfloat16).reshape(2, rows, w_cols)
        y_remote(n, quarter).start()
        y_local(n, quarter).start()
        return carry

    lax.fori_loop(0, chips, gather_near, 0)
    ob_wait(ob.at[far, 1 - core], ob_recv.at[far, 1])
    lax.fori_loop(0, chips, finish, 0)
    for n in range(chips):
        y_remote(n, quarter_of(n)).wait()
        y_local(n, quarter_of(n)).wait()
    for c in x_sends + kv_sends + wo_sends + ob_sends:
        c.wait_send()


def layer(sp_size, tp_size, heads, x_part, w_q, w_k, w_v, w_o):
    kv_loc, group, head_dim = heads
    rows, d_model = x_part.shape
    chunk = 2 * rows
    tiles = group * chunk // TILE
    width = kv_loc * head_dim
    chips = sp_size // 2
    quarter = d_model // sp_size
    f32, bf16 = jnp.float32, jnp.bfloat16
    dma = pltpu.SemaphoreType.DMA
    return pl.pallas_call(
        functools.partial(layer_kernel, (sp_size, tp_size) + heads),
        name="layer",
        out_shape=jax.ShapeDtypeStruct(x_part.shape, bf16),
        in_specs=[pl.BlockSpec(memory_space=pl.ANY)] * 5,
        out_specs=pl.BlockSpec(memory_space=pl.ANY),
        scratch_shapes=[
            pltpu.VMEM((2, WEIGHT_ROWS) + w_q.shape[1:], bf16),
            pltpu.VMEM((2, WEIGHT_ROWS) + w_k.shape[1:], bf16),
            pltpu.VMEM((2, WEIGHT_ROWS) + w_v.shape[1:], bf16),
            pltpu.VMEM((4, 2, rows // 2, d_model), bf16),
            pltpu.VMEM((d_model, group * width), bf16),
            pltpu.VMEM((d_model, 2 * width), bf16),
            pltpu.VMEM((2, kv_loc, group * chunk, head_dim), bf16),
            pltpu.VMEM((sp_size, tp_size, rows, 2 * width), bf16),
            pltpu.VMEM((2, kv_loc, tiles, 1, TILE), f32),
            pltpu.VMEM((2, kv_loc, tiles, 1, TILE), f32),
            pltpu.VMEM((2, kv_loc, tiles, head_dim, TILE), f32),
            pltpu.VMEM((2, chunk, TILE), f32),
            pltpu.VMEM((tp_size, chips, SUBS, w_o.shape[0] // SUBS, quarter), bf16),
            pltpu.VMEM((tp_size, rows, w_o.shape[0]), bf16),
            pltpu.VMEM((tp_size, 2, rows, w_o.shape[0]), bf16),
            pltpu.VMEM((2, rows // 2, w_o.shape[0]), bf16),
            pltpu.VMEM((chips, 2 * rows, quarter), f32),
            pltpu.VMEM((chips, 2, rows, quarter), bf16),
            dma((2,)), dma((2, 3)), dma((6,)), dma((4, 2)), dma((28,)), dma((sp_size, tp_size)),
            dma((chips, SUBS)), dma((48,)), dma((tp_size, chips, SUBS)), dma((10,)), dma((tp_size, 2)), dma((2,)), dma((2,)), dma((chips,)), dma((chips,)), dma((chips,)),
        ],
        compiler_params=pltpu.CompilerParams(collective_id=1, has_side_effects=True, vmem_limit_bytes=62 << 20),
    )(x_part, w_q, w_k, w_v, w_o)


def solution(mesh):
    sp_size, tp_size = mesh.shape["sp"], mesh.shape["tp"]

    def local_attn(x_part, w_query, w_key, w_value, w_out):
        d_model = x_part.shape[1]
        heads_loc, head_dim = w_query.shape[1], w_query.shape[2]
        kv_loc = w_key.shape[1]
        w_o = w_out.reshape(-1, d_model)
        return layer(sp_size, tp_size, (kv_loc, heads_loc // kv_loc, head_dim), x_part, w_query, w_key, w_value, w_o)

    return jax.shard_map(local_attn, mesh=mesh, in_specs=(P(("dp", "sp", "tp"), None), P(None, "tp", None), P(None, "tp", None), P(None, "tp", None), P("tp", None, None)), out_specs=P(("dp", "sp", "tp"), None), check_vma=False)
```

```python
import functools

import jax
import jax.numpy as jnp
from jax import lax
from jax.experimental import pallas as pl
from jax.experimental.pallas import tpu as pltpu
from jax.sharding import PartitionSpec as P

WINDOW = 4096
NEG_BIG = -1e30
LOG2E = 1.4426950408889634
TILE = 768
WEIGHT_ROWS = 512
MESH = pl.DeviceIdType.MESH
NT = (((1,), (1,)), ((), ()))
NN = (((1,), (0,)), ((), ()))
SUBS = 4
WEIGHT_EVENTS = [(3, ((3, 0), (3, 3))), (5, ((3, 1), (3, 2))), (8, ((1, 3), (2, 0)))]
ITEMS = [(dx, flip, f) for group in ([(0, 0)], [(0, 1)], [(-1, 0), (1, 0)], [(-1, 1), (1, 1)], [(2, 0)], [(2, 1)]) for f in (0, 1) for dx, flip in group]


def layer_kernel(dims, x_in, wq_in, wk_in, wv_in, wo_in, out, raw_q, raw_k, raw_v, xs, wq, wkv, q_s, kv, m_s, l_s, acc_s, s_s, wo, o_s, ob, via, total_s, y_s,
                 load_sem, raw_sem, x_send, x_recv, kv_send, kv_recv, wo_load, wo_send, wo_recv, ob_send, ob_recv, via_recv, far_recv, y_send, y_recv, y_store):
    sp_size, tp_size, kv_loc, group, head_dim = dims
    chips = sp_size // 2
    rows, half = 2 * xs.shape[2], xs.shape[2]
    chunk = 2 * rows
    cols = group * chunk
    tiles = cols // TILE
    width = kv_loc * head_dim
    scale = head_dim ** -0.5 * LOG2E
    me, my_tp = lax.axis_index("sp"), lax.axis_index("tp")
    core, chip = lax.rem(me, 2), me // 2

    def rank(dx, flip):
        c = core if flip == 0 else 1 - core
        return 2 * lax.rem(chip + dx + chips, chips) + c

    partner, right, left, opp = rank(0, 1), rank(1, 0), rank(-1, 0), rank(2, 0)
    up, down, far = (lax.rem(my_tp + d, tp_size) for d in (1, tp_size - 1, 2))
    tps = (my_tp, down, up, far)

    barrier = pltpu.get_barrier_semaphore()
    peers = [{"sp": partner}, {"sp": right}, {"sp": left}, {"tp": up}, {"tp": down}]
    for peer in peers:
        pl.semaphore_signal(barrier, inc=1, device_id=peer, device_id_type=MESH)
    loads = [pltpu.make_async_copy(x_in.at[pl.ds(h * half, half)], xs.at[0, h], load_sem.at[h]) for h in (0, 1)]
    for c in loads:
        c.start()
    step_rows = raw_q.shape[1]
    w_chunks = xs.shape[3] // step_rows
    raw = ((wq_in, raw_q, wq, 0), (wk_in, raw_k, wkv, 0), (wv_in, raw_v, wkv, width))

    def raw_load(n, k):
        return pltpu.make_async_copy(raw[k][0].at[pl.ds(pl.multiple_of(n * step_rows, step_rows), step_rows)], raw[k][1].at[lax.rem(n, 2)], raw_sem.at[lax.rem(n, 2), k])

    def flatten_weights():
        def body(n, carry):
            rows_n = pl.ds(pl.multiple_of(n * step_rows, step_rows), step_rows)
            for k, (_, src, dst, lane) in enumerate(raw):
                raw_load(n, k).wait()
                flat = src[lax.rem(n, 2)].reshape(step_rows, src.shape[2] * src.shape[3])
                dst[rows_n, lane:lane + flat.shape[1]] = flat

                @pl.when(n + 2 < w_chunks)
                def _():
                    raw_load(n + 2, k).start()
            return carry

        lax.fori_loop(0, w_chunks, body, 0)

    for n in (0, 1):
        for k in range(3):
            raw_load(n, k).start()
    w_rows, w_cols = wo.shape[3], wo.shape[4]

    def columns(quarter):
        return pl.ds(pl.multiple_of((core * chips + quarter) * w_cols, w_cols), w_cols)

    wo_loads = [pltpu.make_async_copy(wo_in.at[pl.ds(h * w_rows, w_rows), columns(lax.rem(chip + d, chips))],
                                      wo.at[my_tp, lax.rem(chip + d, chips), h], wo_load.at[d, h]) for d in range(chips) for h in range(SUBS)]
    for c in wo_loads:
        c.start()
    pl.semaphore_wait(barrier, len(peers))

    def x_piece(src, h, dst, peer, slot):
        return pltpu.make_async_remote_copy(
            src_ref=xs.at[src, h], dst_ref=xs.at[dst, h], send_sem=x_send.at[slot], recv_sem=x_recv.at[dst, h],
            device_id={"tp": peer}, device_id_type=MESH)

    x_sends = [x_piece(0, 0, 1, up, 0), x_piece(0, 1, 1, down, 1), x_piece(0, 1, 2, up, 2), x_piece(0, 0, 2, down, 3),
               x_piece(1, 0, 3, up, 4), x_piece(1, 1, 3, down, 5)]
    owners = ((my_tp, my_tp), (down, up), (up, down), (far, far))

    kv_sends = []

    def kv_copy(src, o, peer):
        copy = pltpu.make_async_remote_copy(
            src_ref=kv.at[src, tps[o]], dst_ref=kv.at[src, tps[o]], send_sem=kv_send.at[len(kv_sends)],
            recv_sem=kv_recv.at[src, tps[o]], device_id={"sp": peer}, device_id_type=MESH)
        kv_sends.append(copy)
        return copy

    own_kv = [[kv_copy(me, o, peer) for peer in (right, left, partner)] for o in range(4)]
    left_kv = [[kv_copy(left, o, peer) for peer in ((right, partner) if o < 2 else (partner,))] for o in range(4)]
    right_kv = [[kv_copy(right, o, peer) for peer in ((left, partner) if o >= 2 else (partner,))] for o in range(4)]
    opp_kv = [[kv_copy(opp, o, partner)] for o in range(4)]

    def start(copies):
        for c in copies:
            c.start()

    def kv_wait(src, o):
        pltpu.make_async_remote_copy(
            src_ref=kv.at[src, tps[o]], dst_ref=kv.at[src, tps[o]], send_sem=kv_send.at[0], recv_sem=kv_recv.at[src, tps[o]],
            device_id={"sp": partner}, device_id_type=MESH).wait_recv()

    def pass_on(side, src, orders):
        for o in orders:
            kv_wait(src, o)
            start(side[o])

    wo_sends = []

    def wo_copy(o, dx, h, peer):
        at = (tps[o], lax.rem(chip + dx + chips, chips), h)
        copy = pltpu.make_async_remote_copy(
            src_ref=wo.at[at], dst_ref=wo.at[at], send_sem=wo_send.at[len(wo_sends)], recv_sem=wo_recv.at[at],
            device_id=peer, device_id_type=MESH)
        wo_sends.append(copy)
        return copy

    def wo_wait(o, dx, h):
        at = (tps[o], lax.rem(chip + dx + chips, chips), h)
        pltpu.make_async_remote_copy(
            src_ref=wo.at[at], dst_ref=wo.at[at], send_sem=wo_send.at[0], recv_sem=wo_recv.at[at],
            device_id={"sp": partner}, device_id_type=MESH).wait_recv()

    to_up, to_down, to_right, to_left = {"tp": up}, {"tp": down}, {"sp": right}, {"sp": left}
    def both_ways(pairs):
        return [c for h in pairs for c in (wo_copy(0, 0, h, to_up), wo_copy(0, 0, SUBS - 1 - h, to_down))]

    wo_first = both_ways((0, 1))
    wo_second = both_ways((2, 3))
    wo_third = [c for h in (0, 1) for c in (wo_copy(1, 0, h, to_up), wo_copy(2, 0, SUBS - 1 - h, to_down))]
    wo_side = {(o, h): [wo_copy(o, 0, h, peer) for peer, direct in ((to_right, (1, 3)), (to_left, (2, 0))) if (o, h) != direct]
               for o in (1, 2, 3) for h in range(SUBS)}
    wo_relay = {(o, h): wo_copy(o, -1 if h < SUBS // 2 else 1, h, to_right if h < SUBS // 2 else to_left)
                for o, subs in ((1, (0, 1)), (2, (3, 2)), (3, (0, 3, 1, 2))) for h in subs}
    wo_last = [c for h in (0, 1) for c in (wo_copy(0, 2, SUBS // 2 + h, to_up), wo_copy(0, 2, h, to_down))]
    wo_last += [wo_copy(0, -1, 3, to_up), wo_copy(0, 1, 0, to_down)]

    def spread(o, h):
        wo_wait(o, 0, h)
        start(wo_side[o, h])

    def relay(o, h):
        wo_wait(o, -1 if h < SUBS // 2 else 1, h)
        wo_relay[o, h].start()

    def project(step):
        x_rows = xs[step].reshape(rows, xs.shape[3])
        kv_rows = jnp.dot(x_rows, wkv[...], preferred_element_type=jnp.float32).astype(jnp.bfloat16)
        for h in (0, 1):
            kv[me, owners[step][h], h * half:(h + 1) * half, :] = kv_rows[h * half:(h + 1) * half]
        for g in range(kv_loc):
            for hh in range(group):
                if hh % 2:
                    continue
                lane = (g * group + hh) * head_dim
                res = jnp.dot(x_rows, wq[:, lane:lane + 2 * head_dim], preferred_element_type=jnp.float32).astype(jnp.bfloat16)
                for h in (0, 1):
                    tp = owners[step][h]
                    for n in (0, 1):
                        base = pl.multiple_of((hh + n) * chunk + lax.rem(tp, 2) * rows + h * half, half)
                        q_s[tp // 2, g, pl.ds(base, half), :] = res[h * half:(h + 1) * half, n * head_dim:(n + 1) * head_dim]

    loads[0].wait()
    loads[1].wait()
    for c in wo_loads[:SUBS]:
        c.wait()
    start(wo_first)
    start(x_sends[:4])
    start(wo_second[:2])
    m_s[...] = jnp.full(m_s.shape, NEG_BIG, jnp.float32)
    l_s[...] = jnp.zeros_like(l_s)
    acc_s[...] = jnp.zeros_like(acc_s)
    flatten_weights()
    spread(1, 0)
    spread(2, 3)
    def steps(step, carry):
        @pl.when(step == 1)
        def _():
            start(own_kv[0])
            spread(1, 1)
            spread(2, 2)
            x_sends[0].wait_recv()
            x_sends[4].start()
            x_sends[1].wait_recv()
            x_sends[5].start()
            start(wo_third)
            start(wo_second[2:])
            pass_on(left_kv, left, (0,))
            pass_on(right_kv, right, (0,))
            for c in wo_loads[SUBS:]:
                c.wait()

        @pl.when(step == 2)
        def _():
            for o, h in ((1, 0), (2, 3), (1, 1), (2, 2)):
                relay(o, h)
            x_sends[2].wait_recv()
            x_sends[3].wait_recv()

        @pl.when(step == 3)
        def _():
            start(own_kv[1])
            start(own_kv[2])
            pass_on(opp_kv, opp, (0,))
            spread(1, 2)
            spread(2, 1)
            x_sends[4].wait_recv()
            x_sends[5].wait_recv()

        for n in range(4):
            @pl.when(step == n)
            def _():
                project(n)
        return carry

    lax.fori_loop(0, 4, steps, 0)
    start(own_kv[3])

    def update(a, src, b, gap, masked):
        todo = [(g, t) for g in range(kv_loc) for t in range(tiles)]

        def block(lane):
            return kv[src, pl.ds(2 * b, 2), :, lane:lane + head_dim].reshape(chunk, head_dim)

        def scores(n):
            g, t = todo[n]
            s_s[n % 2] = lax.dot_general(block(g * head_dim), q_s[a, g, t * TILE:(t + 1) * TILE, :], NT, preferred_element_type=jnp.float32)

        scores(0)
        v_t = [block(width + g * head_dim).T for g in range(kv_loc)]
        for n, (g, t) in enumerate(todo):
            if n + 1 < len(todo):
                scores(n + 1)
            s = s_s[n % 2]
            if masked:
                raw = t * TILE % chunk + lax.broadcasted_iota(jnp.int32, (chunk, TILE), 1)
                q_pos = jnp.where(raw >= chunk, raw - chunk, raw)
                off = gap * chunk + q_pos - lax.broadcasted_iota(jnp.int32, (chunk, TILE), 0)
                s = jnp.where((off >= 0) & (off < WINDOW), s, NEG_BIG)
            m_old = m_s[a, g, t]
            m_new = jnp.maximum(m_old, jnp.max(s, axis=0, keepdims=True))
            p = jnp.exp2((s - m_new) * scale)
            alpha = jnp.exp2((m_old - m_new) * scale)
            m_s[a, g, t] = m_new
            l_s[a, g, t] = l_s[a, g, t] * alpha + jnp.sum(p, axis=0, keepdims=True)
            acc_s[a, g, t] = acc_s[a, g, t] * alpha + lax.dot_general(v_t[g], p.astype(jnp.bfloat16), NN, preferred_element_type=jnp.float32)

    def wait_for(src, orders):
        for o in orders:
            kv_wait(src, o)

    def before(i, past, done):
        near = (0, 1, 2)

        @pl.when((past < 3) & (done >= 3))
        def _():
            pass_on(left_kv, left, (3,))
            pass_on(right_kv, right, (3,))

        for threshold, pieces in WEIGHT_EVENTS:
            @pl.when((past < threshold) & (done >= threshold))
            def _():
                for o, h in pieces:
                    if o == 3:
                        wo_wait(o, 0, h)
                    else:
                        spread(o, h)
                if pieces[0][0] == 3:
                    first, last = (wo_side[piece] for piece in pieces)
                    start([first[0], last[1], last[0], first[1]])

        @pl.when(i == 0)
        def _():
            pass_on(left_kv, left, (1, 2))
            pass_on(right_kv, right, (1, 2))
            start(wo_last)

        @pl.when(i == 2)
        def _():
            wait_for(partner, near)

        @pl.when(i == 3)
        def _():
            wait_for(partner, (3,))

        @pl.when(i == 8)
        def _():
            wait_for(rank(-1, 1), near)
            wait_for(rank(1, 1), near)
            pass_on(opp_kv, opp, (1, 2))

        @pl.when(i == 10)
        def _():
            wait_for(rank(-1, 1), (3,))
            wait_for(rank(1, 1), (3,))
            pass_on(opp_kv, opp, (3,))

        @pl.when(i == 14)
        def _():
            wait_for(rank(2, 1), near)

        @pl.when(i == 15)
        def _():
            wait_for(rank(2, 1), (3,))

    def pick(i, field):
        out = 0
        for n, entry in enumerate(ITEMS):
            if entry[field]:
                out = out + jnp.where(i == n, entry[field], 0)
        return out

    q_ids = (me, 2 * sp_size - 1 - me)

    def item(i, carry):
        past, done = carry
        before(i, past, done)
        past = done
        dx, flip, f = pick(i, 0), pick(i, 1), pick(i, 2)
        own_b = my_tp // 2
        b = own_b + f - 2 * own_b * f
        src = 2 * lax.rem(chip + dx + chips, chips) + core + flip - 2 * core * flip
        k_id = b * (2 * sp_size - 1) + (1 - 2 * b) * src
        for a in range(2):
            gap = q_ids[a] - k_id
            needed = (gap >= 0) & (gap * chunk - chunk + 1 < WINDOW)
            masked = (gap == 0) | (gap * chunk + chunk - 1 >= WINDOW)
            done = done + needed.astype(jnp.int32)

            @pl.when(needed & masked)
            def _():
                update(a, src, b, gap, True)

            @pl.when(needed & jnp.logical_not(masked))
            def _():
                update(a, src, b, gap, False)

        return past, done

    lax.fori_loop(0, len(ITEMS), item, (0, 0))
    relay(3, 0)
    relay(3, 3)

    for a in range(2):
        for g in range(kv_loc):
            for t in range(tiles):
                norm = acc_s[a, g, t] * (1.0 / l_s[a, g, t])
                for u in range(TILE // 64):
                    col = t * TILE + u * 64
                    h, row = g * group + col // chunk, col % chunk
                    if u % 2 == 0:
                        turned = norm[:, u * 64:u * 64 + 128].T.astype(jnp.bfloat16)
                    o_s[2 * a + row // rows, row % rows:row % rows + 64, h * head_dim:(h + 1) * head_dim] = turned[u % 2 * 64:u % 2 * 64 + 64]

    ob_sends = []

    def ob_copy(src, dst, recv, peer):
        copy = pltpu.make_async_remote_copy(
            src_ref=src, dst_ref=dst, send_sem=ob_send.at[len(ob_sends)], recv_sem=recv, device_id=peer, device_id_type=MESH)
        ob_sends.append(copy)
        return copy

    def ob_wait(ref, recv):
        pltpu.make_async_remote_copy(
            src_ref=ref, dst_ref=ref, send_sem=ob_send.at[0], recv_sem=recv, device_id={"sp": partner}, device_id_type=MESH).wait_recv()

    def part(h):
        return pl.ds(h * half, half)

    ob[my_tp, core] = o_s[my_tp]
    start([ob_copy(o_s.at[far, part(0)], via.at[0], via_recv.at[0], to_up), ob_copy(o_s.at[far, part(1)], via.at[1], via_recv.at[1], to_down)])
    start([ob_copy(o_s.at[up], ob.at[my_tp, core], ob_recv.at[my_tp, 0], to_up), ob_copy(o_s.at[down], ob.at[my_tp, core], ob_recv.at[my_tp, 0], to_down)])
    start([ob_copy(ob.at[my_tp, core], ob.at[my_tp, core], ob_recv.at[my_tp, 1], {"sp": partner})])
    def share(source, quarter):
        res = jnp.dot(ob[source].reshape(2 * rows, SUBS * w_rows), wo[source, quarter].reshape(SUBS * w_rows, w_cols), preferred_element_type=jnp.float32)
        return res.reshape(2, rows, w_cols)

    def add_near(n, c):
        quarter = quarter_of(n)
        res = [jnp.dot(ob[source, c], wo[source, quarter].reshape(SUBS * w_rows, w_cols), preferred_element_type=jnp.float32) for source in (down, up)]
        total_s[n, c] = total_s[n, c] + res[0] + res[1]

    def quarter_of(n):
        return lax.rem(chip + jnp.where(n == 1, chips - 1, jnp.where(n == 2, 1, jnp.where(n == 3, 2, 0))), chips)

    def gather_own(n, carry):
        total_s[n] = share(my_tp, quarter_of(n))
        return carry

    for h, source, peer in ((0, down, to_up), (1, up, to_down)):
        ob_wait(via.at[h], via_recv.at[h])
        start([ob_copy(via.at[h], ob.at[source, core, part(h)], far_recv.at[h], peer)])
    relay(3, 1)
    relay(3, 2)
    ob_wait(ob.at[my_tp, 1 - core], ob_recv.at[my_tp, 1])
    lax.fori_loop(0, chips, gather_own, 0)
    for source in (down, up):
        ob_wait(ob.at[source, core], ob_recv.at[source, 0])
        start([ob_copy(ob.at[source, core], ob.at[source, core], ob_recv.at[source, 1], {"sp": partner})])
    far_share = ob_copy(ob.at[far, core], ob.at[far, core], ob_recv.at[far, 1], {"sp": partner})

    def near_rows(n, carry):
        @pl.when(n == 1)
        def _():
            for h in (0, 1):
                ob_wait(ob.at[far, core, part(h)], far_recv.at[h])
            far_share.start()
            for o, h in ((1, 2), (1, 3), (2, 0), (2, 1), (2, 2), (2, 3), (3, 2), (3, 3)):
                wo_wait(o, -1, h)

        @pl.when(n == 2)
        def _():
            for o, h in ((1, 0), (1, 1), (1, 2), (1, 3), (2, 0), (2, 1), (3, 0), (3, 1)):
                wo_wait(o, 1, h)

        add_near(n, core)
        return carry

    lax.fori_loop(0, chips - 1, near_rows, 0)
    for source in (down, up, far):
        ob_wait(ob.at[source, 1 - core], ob_recv.at[source, 1])

    def y_remote(n, quarter):
        return pltpu.make_async_remote_copy(
            src_ref=y_s.at[n, 1 - core], dst_ref=out.at[:, columns(quarter)], send_sem=y_send.at[n], recv_sem=y_recv.at[n],
            device_id={"sp": partner}, device_id_type=MESH)

    def y_local(n, quarter):
        return pltpu.make_async_copy(y_s.at[n, core], out.at[:, columns(quarter)], y_store.at[n])

    def finish(n, carry):
        @pl.when(n == chips - 1)
        def _():
            for o in (1, 2, 3):
                for h in range(SUBS):
                    wo_wait(o, 2, h)
            add_near(n, core)

        add_near(n, 1 - core)
        quarter = quarter_of(n)
        y_s[n] = (total_s[n] + share(far, quarter)).astype(jnp.bfloat16)
        y_remote(n, quarter).start()
        y_local(n, quarter).start()
        return carry

    lax.fori_loop(0, chips, finish, 0)
    for n in range(chips):
        y_remote(n, quarter_of(n)).wait()
        y_local(n, quarter_of(n)).wait()
    for c in x_sends + kv_sends + wo_sends + ob_sends:
        c.wait_send()


def layer(sp_size, tp_size, heads, x_part, w_q, w_k, w_v, w_o):
    kv_loc, group, head_dim = heads
    rows, d_model = x_part.shape
    chunk = 2 * rows
    tiles = group * chunk // TILE
    width = kv_loc * head_dim
    chips = sp_size // 2
    quarter = d_model // sp_size
    f32, bf16 = jnp.float32, jnp.bfloat16
    dma = pltpu.SemaphoreType.DMA
    return pl.pallas_call(
        functools.partial(layer_kernel, (sp_size, tp_size) + heads),
        name="layer",
        out_shape=jax.ShapeDtypeStruct(x_part.shape, bf16),
        in_specs=[pl.BlockSpec(memory_space=pl.ANY)] * 5,
        out_specs=pl.BlockSpec(memory_space=pl.ANY),
        scratch_shapes=[
            pltpu.VMEM((2, WEIGHT_ROWS) + w_q.shape[1:], bf16),
            pltpu.VMEM((2, WEIGHT_ROWS) + w_k.shape[1:], bf16),
            pltpu.VMEM((2, WEIGHT_ROWS) + w_v.shape[1:], bf16),
            pltpu.VMEM((4, 2, rows // 2, d_model), bf16),
            pltpu.VMEM((d_model, group * width), bf16),
            pltpu.VMEM((d_model, 2 * width), bf16),
            pltpu.VMEM((2, kv_loc, group * chunk, head_dim), bf16),
            pltpu.VMEM((sp_size, tp_size, rows, 2 * width), bf16),
            pltpu.VMEM((2, kv_loc, tiles, 1, TILE), f32),
            pltpu.VMEM((2, kv_loc, tiles, 1, TILE), f32),
            pltpu.VMEM((2, kv_loc, tiles, head_dim, TILE), f32),
            pltpu.VMEM((2, chunk, TILE), f32),
            pltpu.VMEM((tp_size, chips, SUBS, w_o.shape[0] // SUBS, quarter), bf16),
            pltpu.VMEM((tp_size, rows, w_o.shape[0]), bf16),
            pltpu.VMEM((tp_size, 2, rows, w_o.shape[0]), bf16),
            pltpu.VMEM((2, rows // 2, w_o.shape[0]), bf16),
            pltpu.VMEM((chips, 2, rows, quarter), f32),
            pltpu.VMEM((chips, 2, rows, quarter), bf16),
            dma((2,)), dma((2, 3)), dma((6,)), dma((4, 2)), dma((28,)), dma((sp_size, tp_size)),
            dma((chips, SUBS)), dma((48,)), dma((tp_size, chips, SUBS)), dma((10,)), dma((tp_size, 2)), dma((2,)), dma((2,)), dma((chips,)), dma((chips,)), dma((chips,)),
        ],
        compiler_params=pltpu.CompilerParams(collective_id=1, has_side_effects=True, vmem_limit_bytes=62 << 20),
    )(x_part, w_q, w_k, w_v, w_o)


def solution(mesh):
    sp_size, tp_size = mesh.shape["sp"], mesh.shape["tp"]

    def local_attn(x_part, w_query, w_key, w_value, w_out):
        d_model = x_part.shape[1]
        heads_loc, head_dim = w_query.shape[1], w_query.shape[2]
        kv_loc = w_key.shape[1]
        w_o = w_out.reshape(-1, d_model)
        return layer(sp_size, tp_size, (kv_loc, heads_loc // kv_loc, head_dim), x_part, w_query, w_key, w_value, w_o)

    return jax.shard_map(local_attn, mesh=mesh, in_specs=(P(("dp", "sp", "tp"), None), P(None, "tp", None), P(None, "tp", None), P(None, "tp", None), P("tp", None, None)), out_specs=P(("dp", "sp", "tp"), None), check_vma=False)
```
